32 devices in a mesh: seq: 8 (over z, y), feat: 4 (over x, core).
Axes of the slice: x: 2, y: 2, z: 4, core: 2. Of those that a mesh axis runs over, the one named last changes fastest.
Arguments:
- hidden_in: bfloat16 [4, 2048, 2048], P(None, 'seq'), may hold values from -6 to 6
- w_query: bfloat16 [2048, 256], replicated, may hold values from -0.125 to 0.125
- w_key: bfloat16 [2048, 256], replicated, may hold values from -0.125 to 0.125
- w_value: bfloat16 [2048, 2048], P(None, 'feat'), may hold values from -0.125 to 0.125
- lengths: int32 [4], replicated, may hold values from 1024 to 2048, as said below
- owners: int32 [4], replicated, may hold values from 0 to 7
Outputs:
- mixed: bfloat16 [4, 2048, 2048], P(None, 'seq', 'feat')
- state_quad: float32 [8, 4, 16, 256, 128], P('seq', None, None, 'feat')
- state_low: float32 [8, 4, 16, 17, 128], P('seq', None, 'feat')
- norm_quad: float32 [8, 4, 16, 256], P('seq', None, None, 'feat')
- norm_low: float32 [8, 4, 16, 17], P('seq', None, 'feat')
The draws below stay inside these ranges and needn't reach their ends.
Inputs may be any that keep to these rules, and one draw needn't show every extreme that they name: `lengths`: every prompt holds 1024 to 2048 live tokens, and some prompt holds exactly 2048. `owners`: several prompts may share a decoding device.
All inputs are finite; a program needn't handle non-finite values.
Results may differ from the reference program's by a relative error of at most 0.0085.
Values may be sent and summed in bfloat16 or wider, within the bound.
A program may use at most 256 MiB of HBM per device.

```python
import jax
import jax.numpy as jnp
from jax import lax

D = 2048
H = 16
HD = 128
FD = 16
PROMPTS = 4
SPAN = 256
LENGTH = 2048
N_SEQ = 8


def draw_lengths(key, part):
    first_key, second_key = jax.random.split(jax.random.fold_in(key, 11))
    drawn = jax.random.randint(first_key, (PROMPTS,), LENGTH // 2, LENGTH + 1)
    longest = jax.random.randint(second_key, (), 0, PROMPTS)
    return jnp.where(jnp.arange(PROMPTS) == longest, LENGTH, drawn).astype(jnp.int32)


def touch_ends(array, stream_key, least, top_value):
    dims = array.shape
    spot = [jax.random.randint(jax.random.fold_in(stream_key, axis), (), 0, dims[axis]) for axis in range(len(dims))]
    array = array.at[tuple(spot)].set(least)
    longest = dims.index(max(dims))
    spot[longest] = (spot[longest] + 1) % dims[longest]
    return array.at[tuple(spot)].set(top_value)


def levels(stream_key, shape, shards, low, largest):
    def one(axis_at, parts):
        draws = jax.random.uniform(jax.random.fold_in(jax.random.fold_in(stream_key, 6), axis_at), (parts,), jnp.float32, low / len(shards), largest / len(shards))
        return jnp.repeat(jnp.exp(draws), shape[axis_at] // parts).reshape((-1,) + (1,) * (len(shape) - axis_at - 1))

    level = one(*shards[0])
    for cut in shards[1:]:
        level = level * one(*cut)
    return level


def noise(own_key, shape, spread, most, cuts=(), held_as=jnp.bfloat16):
    array = jax.random.normal(own_key, shape, jnp.float32) * spread
    if len(cuts) > 0:
        array = levels(own_key, shape, cuts, -0.22, 0.18) * array
    return jnp.clip(array, min=-most, max=most).astype(held_as)


def setup_inputs(seed: int = 0) -> dict:
    streams_of = jax.random.split(jax.random.key(seed), 7)
    hidden_in = noise(streams_of[0], (PROMPTS, LENGTH, D), 1.0, 6.0, ((1, 8),))
    w_query = noise(streams_of[1], (D, H * FD), D ** -0.5, 0.125)
    w_key = noise(streams_of[2], (D, H * FD), D ** -0.5, 0.125)
    w_value = noise(streams_of[3], (D, D), D ** -0.5, 0.125, ((1, 4),))
    lengths = draw_lengths(jax.random.fold_in(streams_of[6], 71), 0)
    owners = touch_ends(jax.random.randint(streams_of[5], (PROMPTS,), 0, N_SEQ), jax.random.fold_in(streams_of[5], 1), 0, N_SEQ - 1).astype(jnp.int32)
    return dict(hidden_in=hidden_in, w_query=w_query, w_key=w_key, w_value=w_value, lengths=lengths, owners=owners)


NORM_FLOOR = 0.0001

def low_features(inputs):
    constant = jnp.ones(inputs.shape[:-1] + (1,), jnp.float32)
    return jnp.concatenate([constant, inputs * FD ** (-0.25)], axis=-1)

def quad_features(leading, inputs):
    products = leading[..., :, None] * inputs[..., None, :]
    return products.reshape(inputs.shape[:-1] + (leading.shape[-1] * inputs.shape[-1],)) * (2.0 * FD) ** (-0.5)

def reference(hidden_in, w_query, w_key, w_value, lengths, owners):
    highest = lax.Precision.HIGHEST
    n_blocks = LENGTH // SPAN

    def per_prompt(prompt_item):
        tokens, length = prompt_item
        queries = jnp.dot(tokens, w_query, preferred_element_type=jnp.float32).astype(jnp.bfloat16)
        key_rows = jnp.dot(tokens, w_key, preferred_element_type=jnp.float32).astype(jnp.bfloat16)
        values = jnp.dot(tokens, w_value, preferred_element_type=jnp.float32).astype(jnp.bfloat16)
        query_blocks = queries.astype(jnp.float32).reshape(n_blocks, SPAN, H, FD)
        key_blocks = key_rows.astype(jnp.float32).reshape(n_blocks, SPAN, H, FD)
        value_blocks = values.astype(jnp.float32).reshape(n_blocks, SPAN, H, HD)
        starts = jnp.arange(n_blocks, dtype=jnp.int32) * SPAN
        causal = (jnp.arange(SPAN)[:, None] >= jnp.arange(SPAN)[None, :]).astype(jnp.float32)

        def advance(carried, block_data):
            state_lo, state_qu, norm_lo, norm_qu = carried
            query_blk, key_blk, value_blk, start = block_data
            positions = start + jnp.arange(SPAN, dtype=jnp.int32)
            live_mask = (positions < length).astype(jnp.float32)
            query_low = low_features(query_blk)
            query_quad = quad_features(query_blk, query_blk)
            key_low = low_features(key_blk) * live_mask[:, None, None]
            key_quad = quad_features(key_blk, key_blk) * live_mask[:, None, None]
            numerator = jnp.einsum('thf,hfd->thd', query_low, state_lo, precision=highest)
            numerator = numerator + jnp.einsum('thf,hfd->thd', query_quad, state_qu, precision=highest)
            denominator = jnp.einsum('thf,hf->th', query_low, norm_lo, precision=highest)
            denominator = denominator + jnp.einsum('thf,hf->th', query_quad, norm_qu, precision=highest)
            scores = jnp.einsum('thf,uhf->htu', query_blk, key_blk, precision=highest)
            kernel = 1.0 + scores * FD ** (-0.5) + scores * scores * (0.5 / FD)
            weight = kernel * causal[None, :, :] * live_mask[None, None, :]
            numerator = numerator + jnp.einsum('htu,uhd->thd', weight, value_blk, precision=highest)
            denominator = denominator + lax.optimization_barrier(jnp.sum(weight, axis=2)).T
            attended = numerator / denominator[:, :, None] * live_mask[:, None, None]
            new_carried = (state_lo + jnp.einsum('thf,thd->hfd', key_low, value_blk, precision=highest), state_qu + jnp.einsum('thf,thd->hfd', key_quad, value_blk, precision=highest), norm_lo + lax.optimization_barrier(jnp.sum(key_low, axis=0)), norm_qu + lax.optimization_barrier(jnp.sum(key_quad, axis=0)))
            return (new_carried, attended.reshape(SPAN, H * HD))
        initial = (jnp.zeros((H, FD + 1, HD), jnp.float32), jnp.zeros((H, FD * FD, HD), jnp.float32), jnp.zeros((H, FD + 1), jnp.float32), jnp.zeros((H, FD * FD), jnp.float32))
        finals, attended = lax.scan(advance, initial, (query_blocks, key_blocks, value_blocks, starts))
        attended = attended.reshape(LENGTH, H * HD)
        mean_square = lax.optimization_barrier(jnp.mean(attended * attended, axis=-1))
        mixed = (attended * lax.rsqrt(mean_square + NORM_FLOOR)[:, None]).astype(jnp.bfloat16)
        return (mixed, finals)
    mixed, finals = lax.map(per_prompt, (hidden_in, lengths))
    final_low, final_quad, final_lnorm, final_qnorm = finals
    owner_table = (jnp.arange(N_SEQ, dtype=jnp.int32)[:, None] == owners[None, :]).astype(jnp.float32)
    state_quad = owner_table[:, :, None, None, None] * final_quad[None]
    state_low = owner_table[:, :, None, None, None] * final_low[None]
    norm_quad = owner_table[:, :, None, None] * final_qnorm[None]
    norm_low = owner_table[:, :, None, None] * final_lnorm[None]
    return (mixed, state_quad, state_low, norm_quad, norm_low)
```

```python
import functools

import jax
import jax.numpy as jnp
from jax import lax
from jax.experimental import pallas as pl
from jax.experimental.pallas import tpu as pltpu
from jax.sharding import PartitionSpec as P

H = 16
FD = 16
NORM_FLOOR = 0.0001
LANES = 128
BF = jnp.bfloat16
F32 = jnp.float32
LIN = 128
FAR = 144
ONE = 152
LIVE_ROWS = 153

NN = (((1,), (0,)), ((), ()))
NT = (((1,), (1,)), ((), ()))
TN = (((0,), (0,)), ((), ()))


def dot(a, b, dims=NN, precision=None):
    return lax.dot_general(a, b, dims, preferred_element_type=F32, precision=precision)


def iota(shape, axis):
    return lax.broadcasted_iota(jnp.int32, shape, axis)


def features(t, rows, weights):
    diag, off, lin = weights
    tokens = t.shape[1]
    blocks = [t * t * diag if diag != 1.0 else t * t]
    scaled = t * off if off != 1.0 else t
    for o in range(1, FD // 2):
        blocks.append(scaled * pltpu.roll(t, FD - o, 0))
    blocks.append(t * lin if lin != 1.0 else t)
    blocks.append(scaled[: FD // 2] * t[FD // 2 :])
    blocks.append((iota((rows - ONE, tokens), 0) == 0).astype(F32))
    return jnp.concatenate(blocks, axis=0)


def pick_matrix(first_row, count, rows):
    r = iota((count, rows), 0) + first_row
    c = iota((count, rows), 1)
    i, j = r >> 4, r & 15
    o = (j - i) & 15
    place = jnp.where(
        o < 8, o * FD + i, jnp.where(o == 8, FAR + jnp.minimum(i, j), (FD - o) * FD + j)
    )
    return (place == c)


def kernel(cfg, len_ref, x_hbm, wq_hbm, wk_hbm, wv_hbm,
           mixed, quad_out, low_out, nq_out, nl_out,
           hid, wqk, wv, qs, ks, vs, nd, part, got, presend, pre, totsend, tot,
           zsend, zgot, tsend, sqsend, sqgot, ztsend, ztgot,
           in_sem, s1, r1, sz, rz, s2, r2, s3, r3, s4, r4, s5, r5, s6, r6):
    n, nf, npr, span, heads, rows, chunk = cfg
    me, fi = lax.axis_index("seq"), lax.axis_index("feat")
    own = heads * FD
    cpp = n // npr
    head_dim = vs.shape[2] // heads

    base = pl.multiple_of((fi * own // LANES) * LANES, LANES)
    loads = [
        pltpu.make_async_copy(wq_hbm.at[:, pl.ds(base, LANES)], wqk.at[:, pl.ds(0, LANES)], in_sem.at[npr]),
        pltpu.make_async_copy(wk_hbm.at[:, pl.ds(base, LANES)], wqk.at[:, pl.ds(LANES, LANES)], in_sem.at[npr + 1]),
        pltpu.make_async_copy(wv_hbm, wv, in_sem.at[npr + 2]),
    ]
    first = me * npr // n + 1

    def prompt_at(step):
        return lax.rem(first + step, npr)

    def hid_copy(p):
        return pltpu.make_async_copy(x_hbm.at[p], hid.at[p], in_sem.at[p])

    loads[0].start()
    loads[1].start()
    hid_copy(prompt_at(0)).start()
    loads[2].start()
    for step in range(1, npr):
        hid_copy(prompt_at(step)).start()

    barrier = pltpu.get_barrier_semaphore()

    @pl.loop(1, n)
    def _(i):
        pl.semaphore_signal(barrier, 1, device_id={"seq": lax.rem(me + i, n)}, device_id_type=pl.DeviceIdType.MESH)

    for i in range(1, nf):
        pl.semaphore_signal(barrier, 1, device_id={"feat": lax.rem(fi + i, nf)}, device_id_type=pl.DeviceIdType.MESH)
    pl.semaphore_wait(barrier, n - 1 + nf - 1)

    def to_seq(src, dst, ssem, rsem, target):
        return pltpu.make_async_remote_copy(
            src_ref=src, dst_ref=dst, send_sem=ssem, recv_sem=rsem,
            device_id={"seq": target}, device_id_type=pl.DeviceIdType.MESH)

    def to_feat(src, dst, ssem, rsem, target):
        return pltpu.make_async_remote_copy(
            src_ref=src, dst_ref=dst, send_sem=ssem, recv_sem=rsem,
            device_id={"feat": target}, device_id_type=pl.DeviceIdType.MESH)

    peer = lax.rem(me + 1, n)
    fpeer = lax.rem(fi + 1, nf)
    for load in loads:
        load.wait()

    def live_row(p):
        return ((iota((1, span), 1) + me * span) < len_ref[p]).astype(F32)

    def own_half(block):
        out = block[:, :own]
        for r in range(1, LANES // own):
            out = jnp.where(lax.rem(fi, LANES // own) == r, block[:, r * own:(r + 1) * own], out)
        return out

    zsend[...] = jnp.zeros_like(zsend)

    def project(step, _):
        p = prompt_at(step)
        hid_copy(p).wait()
        x = hid[p]
        qk = dot(x, wqk[...])
        q = own_half(qk[:, :LANES]).astype(BF)
        k = own_half(qk[:, LANES:]).astype(BF)
        qs[p] = q
        ks[p] = k
        v = dot(x, wv[...]).astype(BF)
        vs[p] = v
        kt = k.astype(F32).T
        live = live_row(p)
        sums = []
        zrow = iota(zsend.shape, 0)
        z = zsend[...]
        for h in range(heads):
            phi = (features(kt[h * FD:(h + 1) * FD], rows, (1.0, 1.0, 1.0)) * live).astype(BF)
            sums.append(dot(phi, v[:, h * head_dim:(h + 1) * head_dim]).astype(BF))
            zh = dot(jnp.ones((npr * heads, span), BF), phi, NT)
            z = jnp.where(zrow == p * heads + h, zh, z)
        zsend[...] = z
        allsums = jnp.concatenate(sums, axis=0)
        for c in range(cpp):
            target = p * cpp + c
            part[target] = allsums[c * chunk:(c + 1) * chunk]

            @pl.when(target != me)
            def _():
                to_seq(part.at[target], got.at[me], s1.at[target], r1.at[me], target).start()

            @pl.when(target == me)
            def _():
                got[me] = allsums[c * chunk:(c + 1) * chunk]
        return 0

    lax.fori_loop(0, npr, project, 0)

    zgot[me] = zsend[...]

    @pl.loop(1, n)
    def _(i):
        target = lax.rem(me + i, n)
        to_seq(zsend, zgot.at[me], sz.at[i], rz.at[me], target).start()

    def inner(p, _):
        causal = iota((span, span), 0) >= iota((span, span), 1)
        keep = jnp.where(causal, live_row(p), 0.0)
        ones = jnp.ones((span, head_dim), BF)
        for h in range(heads):
            s = dot(qs[p, :, h * FD:(h + 1) * FD], ks[p, :, h * FD:(h + 1) * FD], NT)
            w = ((1.0 + s * (FD ** -0.5 + s * (0.5 / FD))) * keep).astype(BF)
            vv = jnp.concatenate([vs[p, :, h * head_dim:(h + 1) * head_dim], ones], axis=1)
            nd[p, h] = dot(w, vv)
        return 0

    lax.fori_loop(0, npr // 2, inner, 0)

    def scan(s, acc):
        @pl.when(s != me)
        def _():
            to_seq(part.at[s], got.at[s], s1.at[s], r1.at[s], peer).wait_recv()
        presend[s] = acc.astype(BF)
        return acc + got[s].astype(F32)

    total = lax.fori_loop(0, n, scan, jnp.zeros((chunk, head_dim), F32))
    totsend[...] = total.astype(BF)
    tot[me] = total.astype(BF)
    pre[me] = presend[me]

    @pl.loop(1, n)
    def _(i):
        target = lax.rem(me + i, n)
        to_seq(presend.at[target], pre.at[me], s2.at[i], r2.at[me], target).start()

    @pl.loop(1, n)
    def _(i):
        target = lax.rem(me + i, n)
        to_seq(totsend, tot.at[me], s3.at[i], r3.at[me], target).start()

    lax.fori_loop(npr // 2, npr, inner, 0)

    zpre = jnp.zeros(zsend.shape, F32)
    ztot = jnp.zeros(zsend.shape, F32)

    def zsum(s, carry):
        zp, zt = carry

        @pl.when(s != me)
        def _():
            to_seq(zsend, zgot.at[s], sz.at[0], rz.at[s], peer).wait_recv()
        part_z = zgot[s]
        return zp + jnp.where(s < me, part_z, 0.0), zt + part_z

    zpre, ztot = lax.fori_loop(0, n, zsum, (zpre, ztot))
    ztsend[...] = ztot
    ztgot[fi] = ztot
    for i in range(1, nf):
        to_feat(ztsend, ztgot.at[fi], s6.at[i], r6.at[fi], lax.rem(fi + i, nf)).start()

    @pl.loop(1, n)
    def _(i):
        src = lax.rem(me + i, n)
        to_seq(presend.at[src], pre.at[src], s2.at[i], r2.at[src], peer).wait_recv()

    zpre_ref = zsend

    @pl.loop(1, n)
    def _(i):
        to_seq(zsend, zgot.at[me], sz.at[i], rz.at[me], peer).wait_send()

    zpre_ref[...] = zpre
    sqsend[...] = jnp.zeros_like(sqsend)
    weights = (0.5 / FD, 1.0 / FD, FD ** -0.5)

    def outer(p, _):
        qt = qs[p].astype(F32).T
        state = jnp.concatenate([pre[p * cpp + c] for c in range(cpp)], axis=0)
        live = (iota((span, 1), 0) + me * span < len_ref[p]).astype(F32)
        earlier = jnp.minimum(me * span, len_ref[p]).astype(F32)
        sq = jnp.zeros((sqsend.shape[0], span), F32)
        for h in range(heads):
            phi = features(qt[h * FD:(h + 1) * FD], rows, weights).astype(BF)
            zr = zpre_ref[pl.ds(p * heads + h, 1), :]
            zr = jnp.where(iota(zr.shape, 1) == ONE, 0.0, zr)
            zb = jnp.broadcast_to(zr, (head_dim, rows)).astype(BF)
            phit = phi.T
            num = dot(phit, state[h * rows:(h + 1) * rows]) + nd[p, h, :, :head_dim]
            den = dot(phit, zb, NT) + nd[p, h, :, head_dim:] + earlier
            att = num / den * live
            nd[p, h, :, :head_dim] = att
            sq = sq + dot(jnp.ones((sqsend.shape[0], head_dim), BF), (att * att).astype(BF), NT)
        sqsend[...] = jnp.where(iota(sq.shape, 0) == p, sq, sqsend[...])
        return 0

    lax.fori_loop(0, npr, outer, 0)

    sqgot[fi] = sqsend[...]
    for i in range(1, nf):
        to_feat(sqsend, sqgot.at[fi], s4.at[i], r4.at[fi], lax.rem(fi + i, nf)).start()

    @pl.loop(1, n)
    def _(i):
        src = lax.rem(me + i, n)
        to_seq(totsend, tot.at[src], s3.at[i], r3.at[src], peer).wait_recv()

    per = FD * FD // nf
    pick = pick_matrix(0, FD * FD, rows).astype(BF)

    def spread(p, _):
        state = jnp.concatenate([tot[p * cpp + c] for c in range(cpp)], axis=0)
        for h in range(heads):
            mine = state[h * rows:(h + 1) * rows]
            full = dot(pick, mine).astype(BF)
            for f in range(nf):
                tsend[f, p, h] = full[f * per:(f + 1) * per]
            tail = mine[LIN:].astype(F32)
            low_out[p, h] = jnp.concatenate(
                [tail[ONE - LIN:ONE - LIN + 1], tail[:FD] * FD ** -0.25], axis=0)
        return 0

    lax.fori_loop(0, npr, spread, 0)
    for i in range(1, nf):
        target = lax.rem(fi + i, nf)
        to_feat(tsend.at[target], quad_out.at[fi], s5.at[i], r5.at[fi], target).start()
    quad_out[fi] = tsend[fi]

    for i in range(1, nf):
        src = lax.rem(fi + i, nf)
        to_feat(sqsend, sqgot.at[src], s4.at[i], r4.at[src], fpeer).wait_recv()
    squares = sqgot[0]
    for f in range(1, nf):
        squares = squares + sqgot[f]
    width = nf * heads * head_dim
    mean = squares * (1.0 / width) + NORM_FLOOR
    inv = lax.rsqrt(mean)
    zsq = sqsend.shape[0]

    for p in range(npr):
        col = jnp.broadcast_to(inv[p:p + 1], (LANES, span)).T
        for h in range(heads):
            mixed[p, :, h * head_dim:(h + 1) * head_dim] = (nd[p, h, :, :head_dim] * col).astype(BF)

    for i in range(1, nf):
        src = lax.rem(fi + i, nf)
        to_feat(ztsend, ztgot.at[src], s6.at[i], r6.at[src], fpeer).wait_recv()
    own_pick = pick_matrix(fi * per, per, rows).astype(F32)
    for f in range(nf):
        nq = dot(ztgot[f], own_pick, NT, lax.Precision.HIGHEST) * (2.0 * FD) ** -0.5
        for p in range(npr):
            nq_out[p, f * heads:(f + 1) * heads] = nq[p * heads:(p + 1) * heads]
    lr, lc = iota((FD + 1, rows), 0), iota((FD + 1, rows), 1)
    low_pick = jnp.where(lr == 0, (lc == ONE).astype(F32), (lc == LIN - 1 + lr).astype(F32) * FD ** -0.25)
    nl = dot(ztgot[fi], low_pick, NT, lax.Precision.HIGHEST)
    for p in range(npr):
        nl_out[p] = nl[p * heads:(p + 1) * heads]

    for i in range(1, nf):
        src = lax.rem(fi + i, nf)
        to_feat(tsend.at[src], quad_out.at[src], s5.at[i], r5.at[src], fpeer).wait_recv()

    @pl.loop(0, n)
    def _(t):
        @pl.when(t != me)
        def _():
            to_seq(part.at[t], got.at[me], s1.at[t], r1.at[me], peer).wait_send()

    @pl.loop(1, n)
    def _(i):
        target = lax.rem(me + i, n)
        to_seq(presend.at[target], pre.at[me], s2.at[i], r2.at[me], peer).wait_send()
        to_seq(totsend, tot.at[me], s3.at[i], r3.at[me], peer).wait_send()

    for i in range(1, nf):
        to_feat(sqsend, sqgot.at[fi], s4.at[i], r4.at[fi], fpeer).wait_send()
        to_feat(tsend.at[lax.rem(fi + i, nf)], quad_out.at[fi], s5.at[i], r5.at[fi], fpeer).wait_send()
        to_feat(ztsend, ztgot.at[fi], s6.at[i], r6.at[fi], fpeer).wait_send()


def body(hidden_in, w_query, w_key, w_value, lengths, owners):
    npr, span, width = hidden_in.shape
    n, nf = lax.axis_size("seq"), lax.axis_size("feat")
    heads = H // nf
    head_dim = width // H
    step = max(n, 16)
    rows = -(-LIVE_ROWS // 8) * 8
    rows = -(-rows // step) * step if rows % step else rows
    chunk = npr * heads * rows // n
    cfg = (n, nf, npr, span, heads, rows, chunk)
    per = FD * FD // nf
    dma = pltpu.SemaphoreType.DMA
    vm = pltpu.VMEM
    ph = npr * heads
    out = pl.pallas_call(
        functools.partial(kernel, cfg),
        out_shape=(
            jax.ShapeDtypeStruct((npr, span, heads * head_dim), BF),
            jax.ShapeDtypeStruct((nf, npr, heads, per, head_dim), BF),
            jax.ShapeDtypeStruct((npr, heads, FD + 1, head_dim), F32),
            jax.ShapeDtypeStruct((npr, H, per), F32),
            jax.ShapeDtypeStruct((npr, heads, FD + 1), F32),
        ),
        in_specs=[pl.BlockSpec(memory_space=pltpu.SMEM)] + [pl.BlockSpec(memory_space=pl.ANY)] * 4,
        out_specs=[pl.BlockSpec(memory_space=pltpu.VMEM)] * 5,
        scratch_shapes=[
            vm((npr, span, width), BF),
            vm((width, 2 * LANES), BF),
            vm((width, heads * head_dim), BF),
            vm((npr, span, heads * FD), BF),
            vm((npr, span, heads * FD), BF),
            vm((npr, span, heads * head_dim), BF),
            vm((npr, heads, span, 2 * head_dim), F32),
            vm((n, chunk, head_dim), BF),
            vm((n, chunk, head_dim), BF),
            vm((n, chunk, head_dim), BF),
            vm((n, chunk, head_dim), BF),
            vm((chunk, head_dim), BF),
            vm((n, chunk, head_dim), BF),
            vm((ph, rows), F32),
            vm((n, ph, rows), F32),
            vm((nf, npr, heads, per, head_dim), BF),
            vm((8, span), F32),
            vm((nf, 8, span), F32),
            vm((ph, rows), F32),
            vm((nf, ph, rows), F32),
            dma((npr + 3,)),
            dma((n,)), dma((n,)), dma((n,)), dma((n,)),
            dma((n,)), dma((n,)), dma((n,)), dma((n,)),
            dma((nf,)), dma((nf,)), dma((nf,)), dma((nf,)), dma((nf,)), dma((nf,)),
        ],
        compiler_params=pltpu.CompilerParams(
            collective_id=0, has_side_effects=True, vmem_limit_bytes=56 * 1024 * 1024
        ),
        name="layer",
    )(lengths, hidden_in, w_query, w_key, w_value)
    mixed, quad, low, nq, nl = out
    owned = (owners == lax.axis_index("seq")).astype(F32)
    quad = jnp.transpose(quad, (1, 0, 2, 3, 4)).reshape(npr, H, per, head_dim).astype(F32)
    state_quad = (owned[:, None, None, None] * (2.0 * FD) ** -0.5 * quad)[None]
    state_low = (owned[:, None, None, None] * low)[None]
    norm_quad = (owned[:, None, None] * nq)[None]
    norm_low = (owned[:, None, None] * nl)[None]
    return (mixed, state_quad, state_low, norm_quad, norm_low)


def solution(mesh):
    placed = (P(None, "seq", None), P(), P(), P(None, "feat"), P(), P())
    return jax.shard_map(
        body,
        mesh=mesh,
        in_specs=placed,
        out_specs=(
            P(None, "seq", "feat"),
            P("seq", None, None, "feat", None),
            P("seq", None, "feat", None, None),
            P("seq", None, None, "feat"),
            P("seq", None, "feat", None),
        ),
        check_vma=False,
    )
```

```python
import functools

import jax
import jax.numpy as jnp
from jax import lax
from jax.experimental import pallas as pl
from jax.experimental.pallas import tpu as pltpu
from jax.sharding import PartitionSpec as P

H = 16
FD = 16
NORM_FLOOR = 0.0001
LANES = 128
BF = jnp.bfloat16
F32 = jnp.float32
LIN = 128
FAR = 144
ONE = 152
LIVE_ROWS = 153

NN = (((1,), (0,)), ((), ()))
NT = (((1,), (1,)), ((), ()))
TN = (((0,), (0,)), ((), ()))


def dot(a, b, dims=NN, precision=None):
    return lax.dot_general(a, b, dims, preferred_element_type=F32, precision=precision)


def iota(shape, axis):
    return lax.broadcasted_iota(jnp.int32, shape, axis)


def features(t, rows, weights):
    diag, off, lin = weights
    tokens = t.shape[1]
    blocks = [t * t * diag if diag != 1.0 else t * t]
    scaled = t * off if off != 1.0 else t
    for o in range(1, FD // 2):
        blocks.append(scaled * pltpu.roll(t, FD - o, 0))
    blocks.append(t * lin if lin != 1.0 else t)
    blocks.append(scaled[: FD // 2] * t[FD // 2 :])
    blocks.append((iota((rows - ONE, tokens), 0) == 0).astype(F32))
    return jnp.concatenate(blocks, axis=0)


def pick_matrix(first_row, count, rows):
    r = iota((count, rows), 0) + first_row
    c = iota((count, rows), 1)
    i, j = r >> 4, r & 15
    o = (j - i) & 15
    place = jnp.where(
        o < 8, o * FD + i, jnp.where(o == 8, FAR + jnp.minimum(i, j), (FD - o) * FD + j)
    )
    return (place == c)


def kernel(cfg, len_ref, x_hbm, wq_hbm, wk_hbm, wv_hbm,
           mixed, quad_out, low_out, nq_out, nl_out,
           hid, wqk, wv, qs, ks, vs, nd, part, mgot, bsend, got, presend, prer, fwd, pre, tot,
           zsend, zgot, tsend, sqsend, sqgot, ztsend, ztgot,
           in_sem, s0, r0, s1, r1, sz, rz, s2, r2, s3, r3, s4, r4, s5, r5, s6, r6, s7, r7, s8, r8):
    n, nf, npr, span, heads, rows, chunk = cfg
    me, fi = lax.axis_index("seq"), lax.axis_index("feat")
    own = heads * FD
    cpp = n // npr
    outer_n = n // 2
    zo, yi = me // 2, lax.rem(me, 2)
    mate = me + 1 - 2 * yi
    zpeer = 2 * lax.rem(zo + 1, outer_n) + yi
    head_dim = vs.shape[2] // heads

    base = pl.multiple_of((fi * own // LANES) * LANES, LANES)
    loads = [
        pltpu.make_async_copy(wq_hbm.at[:, pl.ds(base, LANES)], wqk.at[:, pl.ds(0, LANES)], in_sem.at[npr]),
        pltpu.make_async_copy(wk_hbm.at[:, pl.ds(base, LANES)], wqk.at[:, pl.ds(LANES, LANES)], in_sem.at[npr + 1]),
        pltpu.make_async_copy(wv_hbm, wv, in_sem.at[npr + 2]),
    ]
    first = me * npr // n + 1

    def prompt_at(step):
        return lax.rem(first + step, npr)

    def hid_copy(p):
        return pltpu.make_async_copy(x_hbm.at[p], hid.at[p], in_sem.at[p])

    loads[0].start()
    loads[1].start()
    hid_copy(prompt_at(0)).start()
    loads[2].start()
    for step in range(1, npr):
        hid_copy(prompt_at(step)).start()

    barrier = pltpu.get_barrier_semaphore()

    @pl.loop(1, n)
    def _(i):
        pl.semaphore_signal(barrier, 1, device_id={"seq": lax.rem(me + i, n)}, device_id_type=pl.DeviceIdType.MESH)

    for i in range(1, nf):
        pl.semaphore_signal(barrier, 1, device_id={"feat": lax.rem(fi + i, nf)}, device_id_type=pl.DeviceIdType.MESH)
    pl.semaphore_wait(barrier, n - 1 + nf - 1)

    def to_seq(src, dst, ssem, rsem, target):
        return pltpu.make_async_remote_copy(
            src_ref=src, dst_ref=dst, send_sem=ssem, recv_sem=rsem,
            device_id={"seq": target}, device_id_type=pl.DeviceIdType.MESH)

    def to_feat(src, dst, ssem, rsem, target):
        return pltpu.make_async_remote_copy(
            src_ref=src, dst_ref=dst, send_sem=ssem, recv_sem=rsem,
            device_id={"feat": target}, device_id_type=pl.DeviceIdType.MESH)

    peer = lax.rem(me + 1, n)
    fpeer = lax.rem(fi + 1, nf)
    for load in loads:
        load.wait()

    def live_row(p):
        return ((iota((1, span), 1) + me * span) < len_ref[p]).astype(F32)

    def own_half(block):
        out = block[:, :own]
        for r in range(1, LANES // own):
            out = jnp.where(lax.rem(fi, LANES // own) == r, block[:, r * own:(r + 1) * own], out)
        return out

    zsend[...] = jnp.zeros_like(zsend)

    def project(step, _):
        p = prompt_at(step)
        hid_copy(p).wait()
        x = hid[p]
        qk = dot(x, wqk[...])
        q = own_half(qk[:, :LANES]).astype(BF)
        k = own_half(qk[:, LANES:]).astype(BF)
        qs[p] = q
        ks[p] = k
        v = dot(x, wv[...]).astype(BF)
        vs[p] = v
        kt = k.astype(F32).T
        live = live_row(p)
        sums = []
        zrow = iota(zsend.shape, 0)
        z = zsend[...]
        for h in range(heads):
            phi = (features(kt[h * FD:(h + 1) * FD], rows, (1.0, 1.0, 1.0)) * live).astype(BF)
            sums.append(dot(phi, v[:, h * head_dim:(h + 1) * head_dim]).astype(BF))
            zh = dot(jnp.ones((npr * heads, span), BF), phi, NT)
            z = jnp.where(zrow == p * heads + h, zh, z)
        zsend[...] = z
        allsums = jnp.concatenate(sums, axis=0)
        for c in range(cpp):
            target = p * cpp + c
            part[target] = allsums[c * chunk:(c + 1) * chunk]

            @pl.when(c % 2 != yi)
            def _():
                slot = target // 2
                to_seq(part.at[target], mgot.at[slot], s0.at[slot], r0.at[slot], mate).start()

        @pl.when(step > 0)
        def _():
            pair_up(prompt_at(step - 1))
        return 0

    def pair_up(p):
        for c in range(cpp // 2):
            slot = p * (cpp // 2) + c
            to_seq(bsend.at[slot], mgot.at[slot], s0.at[slot], r0.at[slot], mate).wait_recv()
            both = part[2 * slot + yi].astype(F32) + mgot[slot].astype(F32)
            bsend[slot] = both.astype(BF)

            @pl.when(slot != zo)
            def _():
                to_seq(bsend.at[slot], got.at[zo], s1.at[slot], r1.at[zo], 2 * slot + yi).start()

            @pl.when(slot == zo)
            def _():
                got[zo] = both.astype(BF)

    lax.fori_loop(0, npr, project, 0)

    zgot[me] = zsend[...]

    @pl.loop(1, n)
    def _(i):
        target = lax.rem(me + i, n)
        to_seq(zsend, zgot.at[me], sz.at[i], rz.at[me], target).start()

    def inner(p, _):
        causal = iota((span, span), 0) >= iota((span, span), 1)
        keep = jnp.where(causal, live_row(p), 0.0)
        ones = jnp.ones((span, head_dim), BF)
        for h in range(heads):
            s = dot(qs[p, :, h * FD:(h + 1) * FD], ks[p, :, h * FD:(h + 1) * FD], NT)
            w = ((1.0 + s * (FD ** -0.5 + s * (0.5 / FD))) * keep).astype(BF)
            vv = jnp.concatenate([vs[p, :, h * head_dim:(h + 1) * head_dim], ones], axis=1)
            nd[p, h] = dot(w, vv)
        return 0

    lax.fori_loop(0, 1, inner, 0)
    pair_up(prompt_at(npr - 1))
    lax.fori_loop(1, npr // 2, inner, 0)

    def scan(s, acc):
        @pl.when(s != zo)
        def _():
            to_seq(bsend.at[s], got.at[s], s1.at[s], r1.at[s], zpeer).wait_recv()
        presend[s] = acc.astype(BF)
        return acc + got[s].astype(F32)

    total = lax.fori_loop(0, outer_n, scan, jnp.zeros((chunk, head_dim), F32))
    tot[me] = total.astype(BF)
    prer[zo] = presend[zo]

    @pl.loop(1, outer_n)
    def _(i):
        there = lax.rem(zo + i, outer_n)
        to_seq(presend.at[there], prer.at[zo], s2.at[i], r2.at[zo], 2 * there + yi).start()

    @pl.loop(1, outer_n)
    def _(i):
        there = lax.rem(zo + i, outer_n)
        to_seq(tot.at[me], tot.at[me], s3.at[i], r3.at[zo], 2 * there + yi).start()

    to_seq(tot.at[me], tot.at[me], s8.at[zo], r8.at[zo], mate).start()

    lax.fori_loop(npr // 2, npr, inner, 0)

    zpre = jnp.zeros(zsend.shape, F32)
    ztot = jnp.zeros(zsend.shape, F32)

    def zsum(s, carry):
        zp, zt = carry

        @pl.when(s != me)
        def _():
            to_seq(zsend, zgot.at[s], sz.at[0], rz.at[s], peer).wait_recv()
        part_z = zgot[s]
        return zp + jnp.where(s < me, part_z, 0.0), zt + part_z

    zpre, ztot = lax.fori_loop(0, n, zsum, (zpre, ztot))
    ztsend[...] = ztot
    ztgot[fi] = ztot
    for i in range(1, nf):
        to_feat(ztsend, ztgot.at[fi], s6.at[i], r6.at[fi], lax.rem(fi + i, nf)).start()

    @pl.loop(0, outer_n)
    def _(i):
        there = lax.rem(zo + i, outer_n)

        @pl.when(i > 0)
        def _():
            to_seq(presend.at[there], prer.at[there], s2.at[i], r2.at[there], zpeer).wait_recv()
        t = 2 * there + yi
        before = prer[there].astype(F32)
        mine = part[t].astype(F32)
        theirs = mgot[there].astype(F32)
        fwd[there] = (before + jnp.where(yi == 0, mine, 0.0)).astype(BF)
        pre[t] = (before + jnp.where(yi == 1, theirs, 0.0)).astype(BF)
        to_seq(fwd.at[there], pre.at[t], s7.at[there], r7.at[there], mate).start()

    zpre_ref = zsend

    @pl.loop(1, n)
    def _(i):
        to_seq(zsend, zgot.at[me], sz.at[i], rz.at[me], peer).wait_send()

    zpre_ref[...] = zpre
    sqsend[...] = jnp.zeros_like(sqsend)
    weights = (0.5 / FD, 1.0 / FD, FD ** -0.5)

    def outer(step, _):
        p = lax.rem(zo * npr // outer_n + step, npr)
        for c in range(cpp // 2):
            slot = p * (cpp // 2) + c
            to_seq(fwd.at[slot], pre.at[2 * slot + 1 - yi], s7.at[slot], r7.at[slot], mate).wait_recv()
        qt = qs[p].astype(F32).T
        state = jnp.concatenate([pre[p * cpp + c] for c in range(cpp)], axis=0)
        live = (iota((span, 1), 0) + me * span < len_ref[p]).astype(F32)
        earlier = jnp.minimum(me * span, len_ref[p]).astype(F32)
        sq = jnp.zeros((sqsend.shape[0], span), F32)
        for h in range(heads):
            phi = features(qt[h * FD:(h + 1) * FD], rows, weights).astype(BF)
            zr = zpre_ref[pl.ds(p * heads + h, 1), :]
            zr = jnp.where(iota(zr.shape, 1) == ONE, 0.0, zr)
            zb = jnp.broadcast_to(zr, (head_dim, rows)).astype(BF)
            phit = phi.T
            num = dot(phit, state[h * rows:(h + 1) * rows]) + nd[p, h, :, :head_dim]
            den = dot(phit, zb, NT) + nd[p, h, :, head_dim:] + earlier
            att = num / den * live
            nd[p, h, :, :head_dim] = att
            sq = sq + dot(jnp.ones((sqsend.shape[0], head_dim), BF), (att * att).astype(BF), NT)
        sqsend[...] = jnp.where(iota(sq.shape, 0) == p, sq, sqsend[...])
        for c in range(cpp // 2):
            slot = p * (cpp // 2) + c

            @pl.when(slot != zo)
            def _():
                t = 2 * slot + yi
                to_seq(tot.at[t], tot.at[t], s3.at[slot], r3.at[slot], zpeer).wait_recv()
                to_seq(tot.at[t], tot.at[t], s8.at[slot], r8.at[slot], mate).start()
        return 0

    lax.fori_loop(0, npr, outer, 0)

    sqgot[fi] = sqsend[...]
    for i in range(1, nf):
        to_feat(sqsend, sqgot.at[fi], s4.at[i], r4.at[fi], lax.rem(fi + i, nf)).start()

    per = FD * FD // nf
    pick = pick_matrix(0, FD * FD, rows).astype(BF)

    def spread(step, _):
        p = lax.rem(zo * npr // outer_n + step, npr)
        for c in range(cpp // 2):
            slot = p * (cpp // 2) + c
            t = 2 * slot + 1 - yi
            to_seq(tot.at[t], tot.at[t], s8.at[slot], r8.at[slot], mate).wait_recv()
        state = jnp.concatenate([tot[p * cpp + c] for c in range(cpp)], axis=0)
        for h in range(heads):
            mine = state[h * rows:(h + 1) * rows]
            full = dot(pick, mine).astype(BF)
            for f in range(nf):
                tsend[f, p, h] = full[f * per:(f + 1) * per]
            tail = mine[LIN:].astype(F32)
            low_out[p, h] = jnp.concatenate(
                [tail[ONE - LIN:ONE - LIN + 1], tail[:FD] * FD ** -0.25], axis=0)
        for i in range(1, nf):
            target = lax.rem(fi + i, nf)
            to_feat(tsend.at[target, p], quad_out.at[fi, p], s5.at[i, p], r5.at[fi, p], target).start()
        return 0

    lax.fori_loop(0, npr, spread, 0)
    quad_out[fi] = tsend[fi]

    for i in range(1, nf):
        src = lax.rem(fi + i, nf)
        to_feat(sqsend, sqgot.at[src], s4.at[i], r4.at[src], fpeer).wait_recv()
    squares = sqgot[0]
    for f in range(1, nf):
        squares = squares + sqgot[f]
    width = nf * heads * head_dim
    mean = squares * (1.0 / width) + NORM_FLOOR
    inv = lax.rsqrt(mean)
    zsq = sqsend.shape[0]

    for p in range(npr):
        col = jnp.broadcast_to(inv[p:p + 1], (LANES, span)).T
        for h in range(heads):
            mixed[p, :, h * head_dim:(h + 1) * head_dim] = (nd[p, h, :, :head_dim] * col).astype(BF)

    for i in range(1, nf):
        src = lax.rem(fi + i, nf)
        to_feat(ztsend, ztgot.at[src], s6.at[i], r6.at[src], fpeer).wait_recv()
    own_pick = pick_matrix(fi * per, per, rows).astype(F32)
    for f in range(nf):
        nq = dot(ztgot[f], own_pick, NT, lax.Precision.HIGHEST) * (2.0 * FD) ** -0.5
        for p in range(npr):
            nq_out[p, f * heads:(f + 1) * heads] = nq[p * heads:(p + 1) * heads]
    lr, lc = iota((FD + 1, rows), 0), iota((FD + 1, rows), 1)
    low_pick = jnp.where(lr == 0, (lc == ONE).astype(F32), (lc == LIN - 1 + lr).astype(F32) * FD ** -0.25)
    nl = dot(ztgot[fi], low_pick, NT, lax.Precision.HIGHEST)
    for p in range(npr):
        nl_out[p] = nl[p * heads:(p + 1) * heads]

    for i in range(1, nf):
        src = lax.rem(fi + i, nf)

        @pl.loop(0, npr)
        def _(p):
            to_feat(tsend.at[src, p], quad_out.at[src, p], s5.at[i, p], r5.at[src, p], fpeer).wait_recv()
            to_feat(tsend.at[src, p], quad_out.at[src, p], s5.at[i, p], r5.at[src, p], fpeer).wait_send()
        to_feat(sqsend, sqgot.at[fi], s4.at[i], r4.at[fi], fpeer).wait_send()
        to_feat(ztsend, ztgot.at[fi], s6.at[i], r6.at[fi], fpeer).wait_send()

    @pl.loop(0, outer_n)
    def _(slot):
        t = 2 * slot + yi
        to_seq(part.at[t], mgot.at[slot], s0.at[slot], r0.at[slot], mate).wait_send()
        to_seq(fwd.at[slot], pre.at[t], s7.at[slot], r7.at[slot], mate).wait_send()
        to_seq(tot.at[t], tot.at[t], s8.at[slot], r8.at[slot], mate).wait_send()

        @pl.when(slot != zo)
        def _():
            to_seq(bsend.at[slot], got.at[zo], s1.at[slot], r1.at[zo], zpeer).wait_send()

    @pl.loop(1, outer_n)
    def _(i):
        to_seq(presend.at[i], prer.at[zo], s2.at[i], r2.at[zo], zpeer).wait_send()
        to_seq(tot.at[me], tot.at[me], s3.at[i], r3.at[zo], zpeer).wait_send()


def finish(cfg, own_ref, mixed, quad, low, nq, nl, mixed_out, quad_out, low_out, nq_out, nl_out):
    nf, heads = cfg
    p = pl.program_id(0)
    mask = (own_ref[p] == lax.axis_index("seq")).astype(F32)
    mixed_out[...] = mixed[...]
    for f in range(nf):
        quad_out[0, f * heads:(f + 1) * heads] = quad[f, 0].astype(F32) * (mask * (2.0 * FD) ** -0.5)
    for h in range(heads):
        low_out[0, :, h, :] = low[0, h] * mask
    nq_out[...] = nq[...] * mask
    nl_out[...] = nl[...] * mask


def body(hidden_in, w_query, w_key, w_value, lengths, owners):
    npr, span, width = hidden_in.shape
    n, nf = lax.axis_size("seq"), lax.axis_size("feat")
    heads = H // nf
    head_dim = width // H
    step = max(n, 16)
    rows = -(-LIVE_ROWS // 8) * 8
    rows = -(-rows // step) * step if rows % step else rows
    chunk = npr * heads * rows // n
    cfg = (n, nf, npr, span, heads, rows, chunk)
    per = FD * FD // nf
    dma = pltpu.SemaphoreType.DMA
    vm = pltpu.VMEM
    ph = npr * heads
    out = pl.pallas_call(
        functools.partial(kernel, cfg),
        out_shape=(
            jax.ShapeDtypeStruct((npr, span, heads * head_dim), BF),
            jax.ShapeDtypeStruct((nf, npr, heads, per, head_dim), BF),
            jax.ShapeDtypeStruct((npr, heads, FD + 1, head_dim), F32),
            jax.ShapeDtypeStruct((npr, H, per), F32),
            jax.ShapeDtypeStruct((npr, heads, FD + 1), F32),
        ),
        in_specs=[pl.BlockSpec(memory_space=pltpu.SMEM)] + [pl.BlockSpec(memory_space=pl.ANY)] * 4,
        out_specs=[pl.BlockSpec(memory_space=pltpu.VMEM)] * 5,
        scratch_shapes=[
            vm((npr, span, width), BF),
            vm((width, 2 * LANES), BF),
            vm((width, heads * head_dim), BF),
            vm((npr, span, heads * FD), BF),
            vm((npr, span, heads * FD), BF),
            vm((npr, span, heads * head_dim), BF),
            vm((npr, heads, span, 2 * head_dim), F32),
            vm((n, chunk, head_dim), BF),
            vm((n // 2, chunk, head_dim), BF),
            vm((n // 2, chunk, head_dim), BF),
            vm((n // 2, chunk, head_dim), BF),
            vm((n // 2, chunk, head_dim), BF),
            vm((n // 2, chunk, head_dim), BF),
            vm((n // 2, chunk, head_dim), BF),
            vm((n, chunk, head_dim), BF),
            vm((n, chunk, head_dim), BF),
            vm((ph, rows), F32),
            vm((n, ph, rows), F32),
            vm((nf, npr, heads, per, head_dim), BF),
            vm((8, span), F32),
            vm((nf, 8, span), F32),
            vm((ph, rows), F32),
            vm((nf, ph, rows), F32),
            dma((npr + 3,)),
            dma((n // 2,)), dma((n // 2,)), dma((n // 2,)), dma((n // 2,)), dma((n,)), dma((n,)),
            dma((n // 2,)), dma((n // 2,)), dma((n // 2,)), dma((n // 2,)),
            dma((nf,)), dma((nf,)), dma((nf, npr)), dma((nf, npr)), dma((nf,)), dma((nf,)),
            dma((n // 2,)), dma((n // 2,)), dma((n // 2,)), dma((n // 2,)),
        ],
        compiler_params=pltpu.CompilerParams(
            collective_id=0, has_side_effects=True, vmem_limit_bytes=56 * 1024 * 1024
        ),
        name="layer",
    )(lengths, hidden_in, w_query, w_key, w_value)
    mixed, quad, low, nq, nl = out
    block = pl.BlockSpec
    mixed, quad, low, nq, nl = pl.pallas_call(
        functools.partial(finish, (nf, heads)),
        grid=(npr,),
        out_shape=(
            jax.ShapeDtypeStruct(mixed.shape, BF),
            jax.ShapeDtypeStruct((npr, H, per, head_dim), F32),
            jax.ShapeDtypeStruct((npr, FD + 1, heads, head_dim), F32),
            jax.ShapeDtypeStruct(nq.shape, F32),
            jax.ShapeDtypeStruct(nl.shape, F32),
        ),
        in_specs=[
            block(memory_space=pltpu.SMEM),
            block((1, span, heads * head_dim), lambda p: (p, 0, 0)),
            block((nf, 1, heads, per, head_dim), lambda p: (0, p, 0, 0, 0)),
            block((1, heads, FD + 1, head_dim), lambda p: (p, 0, 0, 0)),
            block((1, H, per), lambda p: (p, 0, 0)),
            block((1, heads, FD + 1), lambda p: (p, 0, 0)),
        ],
        out_specs=[
            block((1, span, heads * head_dim), lambda p: (p, 0, 0)),
            block((1, H, per, head_dim), lambda p: (p, 0, 0, 0)),
            block((1, FD + 1, heads, head_dim), lambda p: (p, 0, 0, 0)),
            block((1, H, per), lambda p: (p, 0, 0)),
            block((1, heads, FD + 1), lambda p: (p, 0, 0)),
        ],
        name="finish",
    )(owners, mixed, quad, low, nq, nl)
    return (mixed, quad[None], jnp.transpose(low, (0, 2, 1, 3))[None], nq[None], nl[None])


def solution(mesh):
    placed = (P(None, "seq", None), P(), P(), P(None, "feat"), P(), P())
    return jax.shard_map(
        body,
        mesh=mesh,
        in_specs=placed,
        out_specs=(
            P(None, "seq", "feat"),
            P("seq", None, None, "feat", None),
            P("seq", None, "feat", None, None),
            P("seq", None, None, "feat"),
            P("seq", None, "feat", None),
        ),
        check_vma=False,
    )
```

```python
import functools

import jax
import jax.numpy as jnp
from jax import lax
from jax.experimental import pallas as pl
from jax.experimental.pallas import tpu as pltpu
from jax.sharding import PartitionSpec as P

H = 16
FD = 16
NORM_FLOOR = 0.0001
LANES = 128
BF = jnp.bfloat16
F32 = jnp.float32
LIN = 128
FAR = 144
ONE = 152
LIVE_ROWS = 153

NN = (((1,), (0,)), ((), ()))
NT = (((1,), (1,)), ((), ()))
TN = (((0,), (0,)), ((), ()))


def dot(a, b, dims=NN, precision=None):
    return lax.dot_general(a, b, dims, preferred_element_type=F32, precision=precision)


def iota(shape, axis):
    return lax.broadcasted_iota(jnp.int32, shape, axis)


def features(t, rows, weights):
    diag, off, lin = weights
    tokens = t.shape[1]
    blocks = [t * t * diag if diag != 1.0 else t * t]
    scaled = t * off if off != 1.0 else t
    for o in range(1, FD // 2):
        blocks.append(scaled * pltpu.roll(t, FD - o, 0))
    blocks.append(t * lin if lin != 1.0 else t)
    blocks.append(scaled[: FD // 2] * t[FD // 2 :])
    blocks.append((iota((rows - ONE, tokens), 0) == 0).astype(F32))
    return jnp.concatenate(blocks, axis=0)


def pick_matrix(first_row, count, rows):
    r = iota((count, rows), 0) + first_row
    c = iota((count, rows), 1)
    i, j = r >> 4, r & 15
    o = (j - i) & 15
    place = jnp.where(
        o < 8, o * FD + i, jnp.where(o == 8, FAR + jnp.minimum(i, j), (FD - o) * FD + j)
    )
    return (place == c)


def kernel(cfg, len_ref, x_hbm, wq_hbm, wk_hbm, wv_hbm,
           mixed, quad_out, low_out, nq_out, nl_out,
           hid, wqk, wv, qs, ks, vs, nd, part, mgot, bsend, got, presend, prer, fwd, pre, tot,
           tsend, sqsend, sqgot, ztsend, ztgot,
           in_sem, s0, r0, s1, r1, s2, r2, s3, r3, s4, r4, s5, r5, s6, r6, s7, r7, s8, r8):
    n, nf, npr, span, heads, rows, sub = cfg
    me, fi = lax.axis_index("seq"), lax.axis_index("feat")
    own = heads * FD
    outer_n = n // 2
    zo, yi = me // 2, lax.rem(me, 2)
    mate = me + 1 - 2 * yi
    zpeer = 2 * lax.rem(zo + 1, outer_n) + yi
    head_dim = vs.shape[2] // heads

    base = pl.multiple_of((fi * own // LANES) * LANES, LANES)
    loads = [
        pltpu.make_async_copy(wq_hbm.at[:, pl.ds(base, LANES)], wqk.at[:, pl.ds(0, LANES)], in_sem.at[npr]),
        pltpu.make_async_copy(wk_hbm.at[:, pl.ds(base, LANES)], wqk.at[:, pl.ds(LANES, LANES)], in_sem.at[npr + 1]),
        pltpu.make_async_copy(wv_hbm, wv, in_sem.at[npr + 2]),
    ]
    last = outer_n - 1

    def hid_copy(p):
        return pltpu.make_async_copy(x_hbm.at[p], hid.at[p], in_sem.at[p])

    loads[0].start()
    loads[1].start()
    hid_copy(0).start()
    loads[2].start()
    for step in range(1, npr):
        hid_copy(step).start()

    barrier = pltpu.get_barrier_semaphore()

    @pl.loop(1, n)
    def _(i):
        pl.semaphore_signal(barrier, 1, device_id={"seq": lax.rem(me + i, n)}, device_id_type=pl.DeviceIdType.MESH)

    for i in range(1, nf):
        pl.semaphore_signal(barrier, 1, device_id={"feat": lax.rem(fi + i, nf)}, device_id_type=pl.DeviceIdType.MESH)
    pl.semaphore_wait(barrier, n - 1 + nf - 1)

    def to_seq(src, dst, ssem, rsem, target):
        return pltpu.make_async_remote_copy(
            src_ref=src, dst_ref=dst, send_sem=ssem, recv_sem=rsem,
            device_id={"seq": target}, device_id_type=pl.DeviceIdType.MESH)

    def to_feat(src, dst, ssem, rsem, target):
        return pltpu.make_async_remote_copy(
            src_ref=src, dst_ref=dst, send_sem=ssem, recv_sem=rsem,
            device_id={"feat": target}, device_id_type=pl.DeviceIdType.MESH)

    peer = lax.rem(me + 1, n)
    fpeer = lax.rem(fi + 1, nf)
    for load in loads:
        load.wait()

    def live_row(p):
        return ((iota((1, span), 1) + me * span) < len_ref[p]).astype(F32)

    def own_half(block):
        out = block[:, :own]
        for r in range(1, LANES // own):
            out = jnp.where(lax.rem(fi, LANES // own) == r, block[:, r * own:(r + 1) * own], out)
        return out

    def project(p, _):
        hid_copy(p).wait()
        x = hid[p]
        qk = dot(x, wqk[...])
        q = own_half(qk[:, :LANES]).astype(BF)
        k = own_half(qk[:, LANES:]).astype(BF)
        qs[p] = q
        ks[p] = k
        v = dot(x, wv[...]).astype(BF)
        vs[p] = v
        kt = k.astype(F32).T
        live = live_row(p)
        sums = []
        tail = rows - ONE
        row = iota((tail, LANES), 0)
        ones = jnp.ones((tail, span), BF)
        gap = jnp.zeros((tail, 2 * LANES - ONE - 8), F32)
        for h in range(heads):
            phi = (features(kt[h * FD:(h + 1) * FD], rows, (1.0, 1.0, 1.0)) * live).astype(BF)
            summed = dot(phi, v[:, h * head_dim:(h + 1) * head_dim])
            zh = dot(ones, phi, NT)
            more = jnp.concatenate([zh[:, LANES:ONE + 8], gap], axis=1)
            end = summed[ONE:] + jnp.where(row == 1, zh[:, :LANES], 0.0) + jnp.where(row == 2, more, 0.0)
            sums.append(jnp.concatenate([summed[:ONE], end], axis=0).astype(BF))
        half = heads // 2
        for c in range(2):
            part[p, c] = jnp.concatenate(sums[c * half:(c + 1) * half], axis=0).reshape(outer_n, sub, head_dim)
        to_seq(part.at[p, 1 - yi], mgot.at[p], s0.at[p], r0.at[p], mate).start()

        @pl.when(p > 1)
        def _():
            pair_up(p - 2)
        return 0

    def pair_up(p):
        to_seq(bsend.at[p], mgot.at[p], s0.at[p], r0.at[p], mate).wait_recv()
        bsend[p] = (part[p, yi].astype(F32) + mgot[p].astype(F32)).astype(BF)
        got[p, zo] = bsend[p, zo]

        @pl.loop(1, outer_n)
        def _(i):
            there = lax.rem(zo + i, outer_n)
            to_seq(bsend.at[p, there], got.at[p, zo], s1.at[p, i], r1.at[p, zo], 2 * there + yi).start()

    def home(p):
        def scan(z, acc):
            @pl.when(z != zo)
            def _():
                to_seq(bsend.at[p, z], got.at[p, z], s1.at[p, z], r1.at[p, z], zpeer).wait_recv()
            presend[p, z] = acc.astype(BF)
            return acc + got[p, z].astype(F32)

        total = lax.fori_loop(0, outer_n, scan, jnp.zeros((sub, head_dim), F32))
        tot[p, yi, zo] = total.astype(BF)
        prer[p, zo] = presend[p, zo]

        @pl.loop(1, outer_n)
        def _(i):
            there = lax.rem(zo + i, outer_n)

            @pl.when(there != 0)
            def _():
                to_seq(presend.at[p, there], prer.at[p, zo], s2.at[p, i], r2.at[p, zo], 2 * there + yi).start()

        @pl.loop(1, outer_n)
        def _(i):
            there = lax.rem(zo + i, outer_n)

            @pl.when(there != last)
            def _():
                to_seq(tot.at[p, yi, zo], tot.at[p, yi, zo], s3.at[p, i], r3.at[p, zo], 2 * there + yi).start()

    def take_prefix(p):
        @pl.when(zo != 0)
        def _():
            @pl.loop(1, outer_n)
            def _(i):
                there = lax.rem(zo + i, outer_n)
                to_seq(presend.at[p, there], prer.at[p, there], s2.at[p, i], r2.at[p, there], zpeer).wait_recv()

        @pl.when(zo == 0)
        def _():
            prer[p] = jnp.zeros(prer.shape[1:], BF)
        before = prer[p].astype(F32)
        fwd[p] = (before + jnp.where(yi == 0, part[p, yi].astype(F32), 0.0)).astype(BF)
        to_seq(fwd.at[p], pre.at[p, yi], s7.at[p], r7.at[p], mate).start()
        pre[p, yi] = (before + jnp.where(yi == 1, mgot[p].astype(F32), 0.0)).astype(BF)

    def take_total(p):
        @pl.when(zo != last)
        def _():
            @pl.loop(1, outer_n)
            def _(i):
                there = lax.rem(zo + i, outer_n)
                to_seq(presend.at[p, there], tot.at[p, yi, there], s3.at[p, i], r3.at[p, there], zpeer).wait_recv()
            to_seq(tot.at[p, yi], tot.at[p, yi], s8.at[p], r8.at[p], mate).start()

        @pl.when(zo == last)
        def _():
            @pl.loop(1, outer_n)
            def _(i):
                there = lax.rem(zo + i, outer_n)
                tot[p, yi, there] = (prer[p, there].astype(F32) + bsend[p, there].astype(F32)).astype(BF)
            to_seq(tot.at[p, yi], tot.at[p, yi], s8.at[p], r8.at[p], mate).start()

    lax.fori_loop(0, npr, project, 0)

    def inner(p, _):
        causal = iota((span, span), 0) >= iota((span, span), 1)
        keep = jnp.where(causal, live_row(p), 0.0)
        ones = jnp.ones((span, head_dim), BF)
        for h in range(heads):
            s = dot(qs[p, :, h * FD:(h + 1) * FD], ks[p, :, h * FD:(h + 1) * FD], NT)
            w = ((1.0 + s * (FD ** -0.5 + s * (0.5 / FD))) * keep).astype(BF)
            vv = jnp.concatenate([vs[p, :, h * head_dim:(h + 1) * head_dim], ones], axis=1)
            nd[p, h] = dot(w, vv)
        return 0

    sqsend[...] = jnp.zeros_like(sqsend)
    weights = (0.5 / FD, 1.0 / FD, FD ** -0.5)

    def joined(ref, p):
        return jnp.concatenate([ref[p, c].reshape(outer_n * sub, head_dim) for c in range(2)], axis=0)

    def zrow_of(state, h):
        block = state[h * rows + LIN:h * rows + ONE + 8].astype(F32)
        return jnp.concatenate([block[ONE + 1 - LIN:ONE + 2 - LIN], block[ONE + 2 - LIN:ONE + 3 - LIN, :ONE + 8 - LANES]], axis=1)

    def outer(p):
        to_seq(fwd.at[p], pre.at[p, 1 - yi], s7.at[p], r7.at[p], mate).wait_recv()
        qt = qs[p].astype(F32).T
        state = joined(pre, p)
        live = (iota((span, 1), 0) + me * span < len_ref[p]).astype(F32)
        earlier = jnp.minimum(me * span, len_ref[p]).astype(F32)
        sq = jnp.zeros((sqsend.shape[0], span), F32)
        for h in range(heads):
            phi = features(qt[h * FD:(h + 1) * FD], rows, weights).astype(BF)
            zr = zrow_of(state, h)
            zr = jnp.where(iota(zr.shape, 1) == ONE, 0.0, zr)
            zb = jnp.broadcast_to(zr, (head_dim, zr.shape[1])).astype(BF)
            phit = phi.T
            num = dot(phit, state[h * rows:(h + 1) * rows]) + nd[p, h, :, :head_dim]
            den = dot(phit[:, :zr.shape[1]], zb, NT) + nd[p, h, :, head_dim:] + earlier
            att = num / den * live
            nd[p, h, :, :head_dim] = att
            sq = sq + dot(jnp.ones((sqsend.shape[0], head_dim), BF), (att * att).astype(BF), NT)
        sqsend[...] = jnp.where(iota(sq.shape, 0) == p, sq, sqsend[...])

    ztsend[...] = jnp.zeros_like(ztsend)
    per = FD * FD // nf
    pick = pick_matrix(0, FD * FD, rows).astype(BF)

    def spread(p):
        to_seq(tot.at[p, yi], tot.at[p, 1 - yi], s8.at[p], r8.at[p], mate).wait_recv()
        state = joined(tot, p)
        zt = ztsend[...]
        zrow = iota(zt.shape, 0)
        for h in range(heads):
            mine = state[h * rows:(h + 1) * rows]
            zr = zrow_of(state, h)
            zr = jnp.where(iota(zr.shape, 1) == ONE, len_ref[p].astype(F32), zr)
            zt = jnp.where(zrow == p * heads + h, zr, zt)
            full = dot(pick, mine).astype(BF)
            for f in range(nf):
                tsend[f, p, h] = full[f * per:(f + 1) * per]
            tail = mine[LIN:].astype(F32)
            low_out[p, h] = jnp.concatenate(
                [tail[ONE - LIN:ONE - LIN + 1], tail[:FD] * FD ** -0.25], axis=0)
        ztsend[...] = zt
        for i in range(1, nf):
            target = lax.rem(fi + i, nf)
            to_feat(tsend.at[target, p], quad_out.at[fi, p], s5.at[i, p], r5.at[fi, p], target).start()

    lax.fori_loop(0, npr // 2, inner, 0)
    pair_up(npr - 2)
    home(0)
    lax.fori_loop(npr // 2, npr, inner, 0)
    for p in range(1, npr - 2):
        home(p)
    for p in range(npr):
        if p == 0:
            pair_up(npr - 1)
        take_prefix(p)
        take_total(p)
        if p + npr - 2 < npr:
            home(p + npr - 2)
        if p > 0:
            outer(p - 1)
            spread(p - 1)
    outer(npr - 1)

    sqgot[fi] = sqsend[...]
    for i in range(1, nf):
        to_feat(sqsend, sqgot.at[fi], s4.at[i], r4.at[fi], lax.rem(fi + i, nf)).start()

    spread(npr - 1)
    zt = ztsend[...]
    ztgot[fi] = zt
    for i in range(1, nf):
        to_feat(ztsend, ztgot.at[fi], s6.at[i], r6.at[fi], lax.rem(fi + i, nf)).start()
    quad_out[fi] = tsend[fi]

    for i in range(1, nf):
        src = lax.rem(fi + i, nf)
        to_feat(sqsend, sqgot.at[src], s4.at[i], r4.at[src], fpeer).wait_recv()
    squares = sqgot[0]
    for f in range(1, nf):
        squares = squares + sqgot[f]
    width = nf * heads * head_dim
    mean = squares * (1.0 / width) + NORM_FLOOR
    inv = lax.rsqrt(mean)
    zsq = sqsend.shape[0]

    for p in range(npr):
        col = jnp.broadcast_to(inv[p:p + 1], (LANES, span)).T
        for h in range(heads):
            mixed[p, :, h * head_dim:(h + 1) * head_dim] = (nd[p, h, :, :head_dim] * col).astype(BF)

    for i in range(1, nf):
        src = lax.rem(fi + i, nf)
        to_feat(ztsend, ztgot.at[src], s6.at[i], r6.at[src], fpeer).wait_recv()
    own_pick = pick_matrix(fi * per, per, ONE + 8).astype(F32)
    for f in range(nf):
        nq = dot(ztgot[f], own_pick, NT, lax.Precision.HIGHEST) * (2.0 * FD) ** -0.5
        for p in range(npr):
            nq_out[p, f * heads:(f + 1) * heads] = nq[p * heads:(p + 1) * heads]
    lr, lc = iota((FD + 1, ONE + 8), 0), iota((FD + 1, ONE + 8), 1)
    low_pick = jnp.where(lr == 0, (lc == ONE).astype(F32), (lc == LIN - 1 + lr).astype(F32) * FD ** -0.25)
    nl = dot(ztgot[fi], low_pick, NT, lax.Precision.HIGHEST)
    for p in range(npr):
        nl_out[p] = nl[p * heads:(p + 1) * heads]

    for i in range(1, nf):
        src = lax.rem(fi + i, nf)

        @pl.loop(0, npr)
        def _(p):
            to_feat(tsend.at[src, p], quad_out.at[src, p], s5.at[i, p], r5.at[src, p], fpeer).wait_recv()
            to_feat(tsend.at[src, p], quad_out.at[src, p], s5.at[i, p], r5.at[src, p], fpeer).wait_send()
        to_feat(sqsend, sqgot.at[fi], s4.at[i], r4.at[fi], fpeer).wait_send()
        to_feat(ztsend, ztgot.at[fi], s6.at[i], r6.at[fi], fpeer).wait_send()

    @pl.loop(0, npr)
    def _(p):
        to_seq(part.at[p, yi], mgot.at[p], s0.at[p], r0.at[p], mate).wait_send()
        to_seq(fwd.at[p], pre.at[p, yi], s7.at[p], r7.at[p], mate).wait_send()
        to_seq(tot.at[p, yi], tot.at[p, yi], s8.at[p], r8.at[p], mate).wait_send()

        @pl.loop(1, outer_n)
        def _(i):
            there = lax.rem(zo + i, outer_n)
            to_seq(bsend.at[p, there], got.at[p, zo], s1.at[p, i], r1.at[p, zo], zpeer).wait_send()

            @pl.when(there != 0)
            def _():
                to_seq(presend.at[p, there], prer.at[p, zo], s2.at[p, i], r2.at[p, zo], zpeer).wait_send()

            @pl.when(there != last)
            def _():
                to_seq(tot.at[p, yi, zo], tot.at[p, yi, zo], s3.at[p, i], r3.at[p, zo], zpeer).wait_send()


def finish(cfg, own_ref, mixed, quad, low, nq, nl, mixed_out, quad_out, low_out, nq_out, nl_out):
    nf, heads = cfg
    p = pl.program_id(0)
    mask = (own_ref[p] == lax.axis_index("seq")).astype(F32)
    mixed_out[...] = mixed[...]
    for f in range(nf):
        quad_out[0, f * heads:(f + 1) * heads] = quad[f, 0].astype(F32) * (mask * (2.0 * FD) ** -0.5)
    for h in range(heads):
        low_out[0, :, h, :] = low[0, h] * mask
    nq_out[...] = nq[...] * mask
    nl_out[...] = nl[...] * mask


def body(hidden_in, w_query, w_key, w_value, lengths, owners):
    npr, span, width = hidden_in.shape
    n, nf = lax.axis_size("seq"), lax.axis_size("feat")
    heads = H // nf
    head_dim = width // H
    step = 16 * n // heads
    rows = -(-LIVE_ROWS // 8) * 8
    rows = -(-rows // step) * step
    sub = heads * rows // n
    cfg = (n, nf, npr, span, heads, rows, sub)
    per = FD * FD // nf
    dma = pltpu.SemaphoreType.DMA
    vm = pltpu.VMEM
    ph = npr * heads
    out = pl.pallas_call(
        functools.partial(kernel, cfg),
        out_shape=(
            jax.ShapeDtypeStruct((npr, span, heads * head_dim), BF),
            jax.ShapeDtypeStruct((nf, npr, heads, per, head_dim), BF),
            jax.ShapeDtypeStruct((npr, heads, FD + 1, head_dim), F32),
            jax.ShapeDtypeStruct((npr, H, per), F32),
            jax.ShapeDtypeStruct((npr, heads, FD + 1), F32),
        ),
        in_specs=[pl.BlockSpec(memory_space=pltpu.SMEM)] + [pl.BlockSpec(memory_space=pl.ANY)] * 4,
        out_specs=[pl.BlockSpec(memory_space=pltpu.VMEM)] * 5,
        scratch_shapes=[
            vm((npr, span, width), BF),
            vm((width, 2 * LANES), BF),
            vm((width, heads * head_dim), BF),
            vm((npr, span, heads * FD), BF),
            vm((npr, span, heads * FD), BF),
            vm((npr, span, heads * head_dim), BF),
            vm((npr, heads, span, 2 * head_dim), F32),
            vm((npr, 2, n // 2, sub, head_dim), BF),
            vm((npr, n // 2, sub, head_dim), BF),
            vm((npr, n // 2, sub, head_dim), BF),
            vm((npr, n // 2, sub, head_dim), BF),
            vm((npr, n // 2, sub, head_dim), BF),
            vm((npr, n // 2, sub, head_dim), BF),
            vm((npr, n // 2, sub, head_dim), BF),
            vm((npr, 2, n // 2, sub, head_dim), BF),
            vm((npr, 2, n // 2, sub, head_dim), BF),
            vm((nf, npr, heads, per, head_dim), BF),
            vm((8, span), F32),
            vm((nf, 8, span), F32),
            vm((ph, ONE + 8), F32),
            vm((nf, ph, ONE + 8), F32),
            dma((npr + 3,)),
            dma((npr,)), dma((npr,)), dma((npr, n // 2)), dma((npr, n // 2)),
            dma((npr, n // 2)), dma((npr, n // 2)), dma((npr, n // 2)), dma((npr, n // 2)),
            dma((nf,)), dma((nf,)), dma((nf, npr)), dma((nf, npr)), dma((nf,)), dma((nf,)),
            dma((npr,)), dma((npr,)), dma((npr,)), dma((npr,)),
        ],
        compiler_params=pltpu.CompilerParams(
            collective_id=0, has_side_effects=True, vmem_limit_bytes=56 * 1024 * 1024
        ),
        name="layer",
    )(lengths, hidden_in, w_query, w_key, w_value)
    mixed, quad, low, nq, nl = out
    block = pl.BlockSpec
    mixed, quad, low, nq, nl = pl.pallas_call(
        functools.partial(finish, (nf, heads)),
        grid=(npr,),
        out_shape=(
            jax.ShapeDtypeStruct(mixed.shape, BF),
            jax.ShapeDtypeStruct((npr, H, per, head_dim), F32),
            jax.ShapeDtypeStruct((npr, FD + 1, heads, head_dim), F32),
            jax.ShapeDtypeStruct(nq.shape, F32),
            jax.ShapeDtypeStruct(nl.shape, F32),
        ),
        in_specs=[
            block(memory_space=pltpu.SMEM),
            block((1, span, heads * head_dim), lambda p: (p, 0, 0)),
            block((nf, 1, heads, per, head_dim), lambda p: (0, p, 0, 0, 0)),
            block((1, heads, FD + 1, head_dim), lambda p: (p, 0, 0, 0)),
            block((1, H, per), lambda p: (p, 0, 0)),
            block((1, heads, FD + 1), lambda p: (p, 0, 0)),
        ],
        out_specs=[
            block((1, span, heads * head_dim), lambda p: (p, 0, 0)),
            block((1, H, per, head_dim), lambda p: (p, 0, 0, 0)),
            block((1, FD + 1, heads, head_dim), lambda p: (p, 0, 0, 0)),
            block((1, H, per), lambda p: (p, 0, 0)),
            block((1, heads, FD + 1), lambda p: (p, 0, 0)),
        ],
        name="finish",
    )(owners, mixed, quad, low, nq, nl)
    return (mixed, quad[None], jnp.transpose(low, (0, 2, 1, 3))[None], nq[None], nl[None])


def solution(mesh):
    placed = (P(None, "seq", None), P(), P(), P(None, "feat"), P(), P())
    return jax.shard_map(
        body,
        mesh=mesh,
        in_specs=placed,
        out_specs=(
            P(None, "seq", "feat"),
            P("seq", None, None, "feat", None),
            P("seq", None, "feat", None, None),
            P("seq", None, None, "feat"),
            P("seq", None, "feat", None),
        ),
        check_vma=False,
    )
```

```python
import functools

import jax
import jax.numpy as jnp
from jax import lax
from jax.experimental import pallas as pl
from jax.experimental.pallas import tpu as pltpu
from jax.sharding import PartitionSpec as P

H = 16
FD = 16
NORM_FLOOR = 0.0001
LANES = 128
BF = jnp.bfloat16
F32 = jnp.float32
LIN = 128
FAR = 144
ONE = 152
LIVE_ROWS = 153

NN = (((1,), (0,)), ((), ()))
NT = (((1,), (1,)), ((), ()))
TN = (((0,), (0,)), ((), ()))


def dot(a, b, dims=NN, precision=None):
    return lax.dot_general(a, b, dims, preferred_element_type=F32, precision=precision)


def iota(shape, axis):
    return lax.broadcasted_iota(jnp.int32, shape, axis)


def features(t, rows, weights):
    diag, off, lin = weights
    tokens = t.shape[1]
    blocks = [t * t * diag if diag != 1.0 else t * t]
    scaled = t * off if off != 1.0 else t
    for o in range(1, FD // 2):
        blocks.append(scaled * pltpu.roll(t, FD - o, 0))
    blocks.append(t * lin if lin != 1.0 else t)
    blocks.append(scaled[: FD // 2] * t[FD // 2 :])
    blocks.append((iota((rows - ONE, tokens), 0) == 0).astype(F32))
    return jnp.concatenate(blocks, axis=0)


def pick_matrix(first_row, count, rows):
    r = iota((count, rows), 0) + first_row
    c = iota((count, rows), 1)
    i, j = r >> 4, r & 15
    o = (j - i) & 15
    place = jnp.where(
        o < 8, o * FD + i, jnp.where(o == 8, FAR + jnp.minimum(i, j), (FD - o) * FD + j)
    )
    return (place == c)


def kernel(cfg, len_ref, x_hbm, wq_hbm, wk_hbm, wv_hbm,
           mixed, quad_out, low_out, nq_out, nl_out,
           hid, wqk, wv, qs, ks, vs, nd, part, mgot, bsend, got, presend, prer, fwd, pre, tot,
           tsend, sqsend, sqgot, ztsend, ztgot,
           in_sem, s0, r0, s1, r1, s2, r2, s3, r3, s4, r4, s5, r5, s6, r6, s7, r7, s8, r8):
    n, nf, npr, span, heads, rows, sub = cfg
    me, fi = lax.axis_index("seq"), lax.axis_index("feat")
    own = heads * FD
    outer_n = n // 2
    zo, yi = me // 2, lax.rem(me, 2)
    mate = me + 1 - 2 * yi
    zpeer = 2 * lax.rem(zo + 1, outer_n) + yi
    head_dim = vs.shape[2] // heads

    base = pl.multiple_of((fi * own // LANES) * LANES, LANES)
    loads = [
        pltpu.make_async_copy(wq_hbm.at[:, pl.ds(base, LANES)], wqk.at[:, pl.ds(0, LANES)], in_sem.at[npr]),
        pltpu.make_async_copy(wk_hbm.at[:, pl.ds(base, LANES)], wqk.at[:, pl.ds(LANES, LANES)], in_sem.at[npr + 1]),
        pltpu.make_async_copy(wv_hbm, wv, in_sem.at[npr + 2]),
    ]
    last = outer_n - 1

    def hid_copy(p):
        return pltpu.make_async_copy(x_hbm.at[p], hid.at[p], in_sem.at[p])

    loads[0].start()
    loads[1].start()
    hid_copy(0).start()
    loads[2].start()
    for step in range(1, npr):
        hid_copy(step).start()

    barrier = pltpu.get_barrier_semaphore()

    @pl.loop(1, n)
    def _(i):
        pl.semaphore_signal(barrier, 1, device_id={"seq": lax.rem(me + i, n)}, device_id_type=pl.DeviceIdType.MESH)

    for i in range(1, nf):
        pl.semaphore_signal(barrier, 1, device_id={"feat": lax.rem(fi + i, nf)}, device_id_type=pl.DeviceIdType.MESH)
    pl.semaphore_wait(barrier, n - 1 + nf - 1)

    def to_seq(src, dst, ssem, rsem, target):
        return pltpu.make_async_remote_copy(
            src_ref=src, dst_ref=dst, send_sem=ssem, recv_sem=rsem,
            device_id={"seq": target}, device_id_type=pl.DeviceIdType.MESH)

    def to_feat(src, dst, ssem, rsem, target):
        return pltpu.make_async_remote_copy(
            src_ref=src, dst_ref=dst, send_sem=ssem, recv_sem=rsem,
            device_id={"feat": target}, device_id_type=pl.DeviceIdType.MESH)

    peer = lax.rem(me + 1, n)
    fpeer = lax.rem(fi + 1, nf)
    for load in loads:
        load.wait()

    def live_row(p):
        return ((iota((1, span), 1) + me * span) < len_ref[p]).astype(F32)

    def own_half(block):
        out = block[:, :own]
        for r in range(1, LANES // own):
            out = jnp.where(lax.rem(fi, LANES // own) == r, block[:, r * own:(r + 1) * own], out)
        return out

    def project(p, _):
        hid_copy(p).wait()
        x = hid[p]
        qk = dot(x, wqk[...])
        q = own_half(qk[:, :LANES]).astype(BF)
        k = own_half(qk[:, LANES:]).astype(BF)
        qs[p] = q
        ks[p] = k
        v = dot(x, wv[...]).astype(BF)
        vs[p] = v
        kt = k.astype(F32).T
        live = live_row(p)
        sums = []
        tail = rows - ONE
        row = iota((tail, LANES), 0)
        ones = jnp.ones((tail, span), BF)
        gap = jnp.zeros((tail, 2 * LANES - ONE - 8), F32)
        for h in range(heads):
            phi = (features(kt[h * FD:(h + 1) * FD], rows, (1.0, 1.0, 1.0)) * live).astype(BF)
            summed = dot(phi, v[:, h * head_dim:(h + 1) * head_dim])
            zh = dot(ones, phi, NT)
            more = jnp.concatenate([zh[:, LANES:ONE + 8], gap], axis=1)
            end = summed[ONE:] + jnp.where(row == 1, zh[:, :LANES], 0.0) + jnp.where(row == 2, more, 0.0)
            sums.append(jnp.concatenate([summed[:ONE], end], axis=0).astype(BF))
        half = heads // 2
        for c in range(2):
            part[p, c] = jnp.concatenate(sums[c * half:(c + 1) * half], axis=0).reshape(outer_n, sub, head_dim)
        to_seq(part.at[p, 1 - yi], mgot.at[p], s0.at[p], r0.at[p], mate).start()

        @pl.when(p > 0)
        def _():
            pair_up(p - 1)
        return 0

    def pair_up(p):
        to_seq(bsend.at[p], mgot.at[p], s0.at[p], r0.at[p], mate).wait_recv()
        bsend[p] = (part[p, yi].astype(F32) + mgot[p].astype(F32)).astype(BF)
        got[p, zo] = bsend[p, zo]

        @pl.loop(1, outer_n)
        def _(i):
            there = lax.rem(zo + i, outer_n)
            to_seq(bsend.at[p, there], got.at[p, zo], s1.at[p, i], r1.at[p, zo], 2 * there + yi).start()

    def home(p):
        def scan(z, acc):
            @pl.when(z != zo)
            def _():
                to_seq(bsend.at[p, z], got.at[p, z], s1.at[p, z], r1.at[p, z], zpeer).wait_recv()
            presend[p, z] = acc.astype(BF)
            return acc + got[p, z].astype(F32)

        total = lax.fori_loop(0, outer_n, scan, jnp.zeros((sub, head_dim), F32))
        tot[p, yi, zo] = total.astype(BF)
        prer[p, zo] = presend[p, zo]

        @pl.loop(1, outer_n)
        def _(i):
            there = lax.rem(zo + i, outer_n)

            @pl.when(there != 0)
            def _():
                to_seq(presend.at[p, there], prer.at[p, zo], s2.at[p, i], r2.at[p, zo], 2 * there + yi).start()

        @pl.loop(1, outer_n)
        def _(i):
            there = lax.rem(zo + i, outer_n)

            @pl.when(there != last)
            def _():
                to_seq(tot.at[p, yi, zo], tot.at[p, yi, zo], s3.at[p, i], r3.at[p, zo], 2 * there + yi).start()

    def take_prefix(p):
        @pl.when(zo != 0)
        def _():
            @pl.loop(1, outer_n)
            def _(i):
                there = lax.rem(zo + i, outer_n)
                to_seq(presend.at[p, there], prer.at[p, there], s2.at[p, i], r2.at[p, there], zpeer).wait_recv()

        @pl.when(zo == 0)
        def _():
            prer[p] = jnp.zeros(prer.shape[1:], BF)
        before = prer[p].astype(F32)
        fwd[p] = (before + jnp.where(yi == 0, part[p, yi].astype(F32), 0.0)).astype(BF)
        to_seq(fwd.at[p], pre.at[p, yi], s7.at[p], r7.at[p], mate).start()
        pre[p, yi] = (before + jnp.where(yi == 1, mgot[p].astype(F32), 0.0)).astype(BF)

    def take_total(p):
        @pl.when(zo != last)
        def _():
            @pl.loop(1, outer_n)
            def _(i):
                there = lax.rem(zo + i, outer_n)
                to_seq(presend.at[p, there], tot.at[p, yi, there], s3.at[p, i], r3.at[p, there], zpeer).wait_recv()
            to_seq(tot.at[p, yi], tot.at[p, yi], s8.at[p], r8.at[p], mate).start()

        @pl.when(zo == last)
        def _():
            @pl.loop(1, outer_n)
            def _(i):
                there = lax.rem(zo + i, outer_n)
                tot[p, yi, there] = (prer[p, there].astype(F32) + bsend[p, there].astype(F32)).astype(BF)
            to_seq(tot.at[p, yi], tot.at[p, yi], s8.at[p], r8.at[p], mate).start()

    lax.fori_loop(0, npr, project, 0)

    def inner(p, _):
        causal = iota((span, span), 0) >= iota((span, span), 1)
        keep = jnp.where(causal, live_row(p), 0.0)
        ones = jnp.ones((span, head_dim), BF)
        for h in range(heads):
            s = dot(qs[p, :, h * FD:(h + 1) * FD], ks[p, :, h * FD:(h + 1) * FD], NT)
            w = ((1.0 + s * (FD ** -0.5 + s * (0.5 / FD))) * keep).astype(BF)
            vv = jnp.concatenate([vs[p, :, h * head_dim:(h + 1) * head_dim], ones], axis=1)
            nd[p, h] = dot(w, vv)
        return 0

    sqsend[...] = jnp.zeros_like(sqsend)
    weights = (0.5 / FD, 1.0 / FD, FD ** -0.5)

    def joined(ref, p):
        return jnp.concatenate([ref[p, c].reshape(outer_n * sub, head_dim) for c in range(2)], axis=0)

    def zrow_of(state, h):
        block = state[h * rows + LIN:h * rows + ONE + 8].astype(F32)
        return jnp.concatenate([block[ONE + 1 - LIN:ONE + 2 - LIN], block[ONE + 2 - LIN:ONE + 3 - LIN, :ONE + 8 - LANES]], axis=1)

    def outer(p):
        to_seq(fwd.at[p], pre.at[p, 1 - yi], s7.at[p], r7.at[p], mate).wait_recv()
        qt = qs[p].astype(F32).T
        state = joined(pre, p)
        live = (iota((span, 1), 0) + me * span < len_ref[p]).astype(F32)
        earlier = jnp.minimum(me * span, len_ref[p]).astype(F32)
        sq = jnp.zeros((sqsend.shape[0], span), F32)
        for h in range(heads):
            phi = features(qt[h * FD:(h + 1) * FD], rows, weights).astype(BF)
            zr = zrow_of(state, h)
            zr = jnp.where(iota(zr.shape, 1) == ONE, 0.0, zr)
            zb = jnp.broadcast_to(zr, (head_dim, zr.shape[1])).astype(BF)
            phit = phi.T
            num = dot(phit, state[h * rows:(h + 1) * rows]) + nd[p, h, :, :head_dim]
            den = dot(phit[:, :zr.shape[1]], zb, NT) + nd[p, h, :, head_dim:] + earlier
            att = num / den * live
            nd[p, h, :, :head_dim] = att
            sq = sq + dot(jnp.ones((sqsend.shape[0], head_dim), BF), (att * att).astype(BF), NT)
        sqsend[...] = jnp.where(iota(sq.shape, 0) == p, sq, sqsend[...])

    ztsend[...] = jnp.zeros_like(ztsend)
    per = FD * FD // nf
    pick = pick_matrix(0, FD * FD, rows).astype(BF)

    def spread(p):
        to_seq(tot.at[p, yi], tot.at[p, 1 - yi], s8.at[p], r8.at[p], mate).wait_recv()
        state = joined(tot, p)
        zt = ztsend[...]
        zrow = iota(zt.shape, 0)
        for h in range(heads):
            mine = state[h * rows:(h + 1) * rows]
            zr = zrow_of(state, h)
            zr = jnp.where(iota(zr.shape, 1) == ONE, len_ref[p].astype(F32), zr)
            zt = jnp.where(zrow == p * heads + h, zr, zt)
            full = dot(pick, mine).astype(BF)
            for f in range(nf):
                tsend[f, p, h] = full[f * per:(f + 1) * per]
            tail = mine[LIN:].astype(F32)
            low_out[p, h] = jnp.concatenate(
                [tail[ONE - LIN:ONE - LIN + 1], tail[:FD] * FD ** -0.25], axis=0)
        ztsend[...] = zt
        for i in range(1, nf):
            target = lax.rem(fi + i, nf)
            to_feat(tsend.at[target, p], quad_out.at[fi, p], s5.at[i, p], r5.at[fi, p], target).start()

    lax.fori_loop(0, npr // 2, inner, 0)
    home(0)
    lax.fori_loop(npr // 2, npr, inner, 0)
    for p in range(1, npr - 2):
        home(p)
    for p in range(npr):
        if p == 0:
            pair_up(npr - 1)
        take_prefix(p)
        take_total(p)
        if p + npr - 2 < npr:
            home(p + npr - 2)
        if p > 0:
            outer(p - 1)
            spread(p - 1)
    outer(npr - 1)

    sqgot[fi] = sqsend[...]
    for i in range(1, nf):
        to_feat(sqsend, sqgot.at[fi], s4.at[i], r4.at[fi], lax.rem(fi + i, nf)).start()

    spread(npr - 1)
    zt = ztsend[...]
    ztgot[fi] = zt
    for i in range(1, nf):
        to_feat(ztsend, ztgot.at[fi], s6.at[i], r6.at[fi], lax.rem(fi + i, nf)).start()
    quad_out[fi] = tsend[fi]

    for i in range(1, nf):
        src = lax.rem(fi + i, nf)
        to_feat(sqsend, sqgot.at[src], s4.at[i], r4.at[src], fpeer).wait_recv()
    squares = sqgot[0]
    for f in range(1, nf):
        squares = squares + sqgot[f]
    width = nf * heads * head_dim
    mean = squares * (1.0 / width) + NORM_FLOOR
    inv = lax.rsqrt(mean)
    zsq = sqsend.shape[0]

    for p in range(npr):
        col = jnp.broadcast_to(inv[p:p + 1], (LANES, span)).T
        for h in range(heads):
            mixed[p, :, h * head_dim:(h + 1) * head_dim] = (nd[p, h, :, :head_dim] * col).astype(BF)

    for i in range(1, nf):
        src = lax.rem(fi + i, nf)
        to_feat(ztsend, ztgot.at[src], s6.at[i], r6.at[src], fpeer).wait_recv()
    own_pick = pick_matrix(fi * per, per, ONE + 8).astype(F32)
    for f in range(nf):
        nq = dot(ztgot[f], own_pick, NT, lax.Precision.HIGHEST) * (2.0 * FD) ** -0.5
        for p in range(npr):
            nq_out[p, f * heads:(f + 1) * heads] = nq[p * heads:(p + 1) * heads]
    lr, lc = iota((FD + 1, ONE + 8), 0), iota((FD + 1, ONE + 8), 1)
    low_pick = jnp.where(lr == 0, (lc == ONE).astype(F32), (lc == LIN - 1 + lr).astype(F32) * FD ** -0.25)
    nl = dot(ztgot[fi], low_pick, NT, lax.Precision.HIGHEST)
    for p in range(npr):
        nl_out[p] = nl[p * heads:(p + 1) * heads]

    for i in range(1, nf):
        src = lax.rem(fi + i, nf)

        @pl.loop(0, npr)
        def _(p):
            to_feat(tsend.at[src, p], quad_out.at[src, p], s5.at[i, p], r5.at[src, p], fpeer).wait_recv()
            to_feat(tsend.at[src, p], quad_out.at[src, p], s5.at[i, p], r5.at[src, p], fpeer).wait_send()
        to_feat(sqsend, sqgot.at[fi], s4.at[i], r4.at[fi], fpeer).wait_send()
        to_feat(ztsend, ztgot.at[fi], s6.at[i], r6.at[fi], fpeer).wait_send()

    @pl.loop(0, npr)
    def _(p):
        to_seq(part.at[p, yi], mgot.at[p], s0.at[p], r0.at[p], mate).wait_send()
        to_seq(fwd.at[p], pre.at[p, yi], s7.at[p], r7.at[p], mate).wait_send()
        to_seq(tot.at[p, yi], tot.at[p, yi], s8.at[p], r8.at[p], mate).wait_send()

        @pl.loop(1, outer_n)
        def _(i):
            there = lax.rem(zo + i, outer_n)
            to_seq(bsend.at[p, there], got.at[p, zo], s1.at[p, i], r1.at[p, zo], zpeer).wait_send()

            @pl.when(there != 0)
            def _():
                to_seq(presend.at[p, there], prer.at[p, zo], s2.at[p, i], r2.at[p, zo], zpeer).wait_send()

            @pl.when(there != last)
            def _():
                to_seq(tot.at[p, yi, zo], tot.at[p, yi, zo], s3.at[p, i], r3.at[p, zo], zpeer).wait_send()


def finish(cfg, own_ref, mixed, quad, low, nq, nl, mixed_out, quad_out, low_out, nq_out, nl_out):
    nf, heads = cfg
    mixed_out[...] = mixed[...]
    count = nq.shape[0]
    for b in range(count):
        mask = (own_ref[pl.program_id(0) * count + b] == lax.axis_index("seq")).astype(F32)
        finish_one(nf, heads, b, mask, quad, low, nq, nl, quad_out, low_out, nq_out, nl_out)


def finish_one(nf, heads, b, mask, quad, low, nq, nl, quad_out, low_out, nq_out, nl_out):
    for f in range(nf):
        quad_out[b, f * heads:(f + 1) * heads] = quad[f, b].astype(F32) * (mask * (2.0 * FD) ** -0.5)
    for h in range(heads):
        low_out[b, :, h, :] = low[b, h] * mask
    nq_out[b] = nq[b] * mask
    nl_out[b] = nl[b] * mask


def body(hidden_in, w_query, w_key, w_value, lengths, owners):
    npr, span, width = hidden_in.shape
    n, nf = lax.axis_size("seq"), lax.axis_size("feat")
    heads = H // nf
    head_dim = width // H
    step = 16 * n // heads
    rows = -(-LIVE_ROWS // 8) * 8
    rows = -(-rows // step) * step
    sub = heads * rows // n
    cfg = (n, nf, npr, span, heads, rows, sub)
    per = FD * FD // nf
    dma = pltpu.SemaphoreType.DMA
    vm = pltpu.VMEM
    ph = npr * heads
    out = pl.pallas_call(
        functools.partial(kernel, cfg),
        out_shape=(
            jax.ShapeDtypeStruct((npr, span, heads * head_dim), BF),
            jax.ShapeDtypeStruct((nf, npr, heads, per, head_dim), BF),
            jax.ShapeDtypeStruct((npr, heads, FD + 1, head_dim), F32),
            jax.ShapeDtypeStruct((npr, H, per), F32),
            jax.ShapeDtypeStruct((npr, heads, FD + 1), F32),
        ),
        in_specs=[pl.BlockSpec(memory_space=pltpu.SMEM)] + [pl.BlockSpec(memory_space=pl.ANY)] * 4,
        out_specs=[pl.BlockSpec(memory_space=pltpu.VMEM)] * 5,
        scratch_shapes=[
            vm((npr, span, width), BF),
            vm((width, 2 * LANES), BF),
            vm((width, heads * head_dim), BF),
            vm((npr, span, heads * FD), BF),
            vm((npr, span, heads * FD), BF),
            vm((npr, span, heads * head_dim), BF),
            vm((npr, heads, span, 2 * head_dim), F32),
            vm((npr, 2, n // 2, sub, head_dim), BF),
            vm((npr, n // 2, sub, head_dim), BF),
            vm((npr, n // 2, sub, head_dim), BF),
            vm((npr, n // 2, sub, head_dim), BF),
            vm((npr, n // 2, sub, head_dim), BF),
            vm((npr, n // 2, sub, head_dim), BF),
            vm((npr, n // 2, sub, head_dim), BF),
            vm((npr, 2, n // 2, sub, head_dim), BF),
            vm((npr, 2, n // 2, sub, head_dim), BF),
            vm((nf, npr, heads, per, head_dim), BF),
            vm((8, span), F32),
            vm((nf, 8, span), F32),
            vm((ph, ONE + 8), F32),
            vm((nf, ph, ONE + 8), F32),
            dma((npr + 3,)),
            dma((npr,)), dma((npr,)), dma((npr, n // 2)), dma((npr, n // 2)),
            dma((npr, n // 2)), dma((npr, n // 2)), dma((npr, n // 2)), dma((npr, n // 2)),
            dma((nf,)), dma((nf,)), dma((nf, npr)), dma((nf, npr)), dma((nf,)), dma((nf,)),
            dma((npr,)), dma((npr,)), dma((npr,)), dma((npr,)),
        ],
        compiler_params=pltpu.CompilerParams(
            collective_id=0, has_side_effects=True, vmem_limit_bytes=56 * 1024 * 1024
        ),
        name="layer",
    )(lengths, hidden_in, w_query, w_key, w_value)
    mixed, quad, low, nq, nl = out
    block = pl.BlockSpec
    group = 2 - npr % 2
    mixed, quad, low, nq, nl = pl.pallas_call(
        functools.partial(finish, (nf, heads)),
        grid=(npr // group,),
        out_shape=(
            jax.ShapeDtypeStruct(mixed.shape, BF),
            jax.ShapeDtypeStruct((npr, H, per, head_dim), F32),
            jax.ShapeDtypeStruct((npr, FD + 1, heads, head_dim), F32),
            jax.ShapeDtypeStruct(nq.shape, F32),
            jax.ShapeDtypeStruct(nl.shape, F32),
        ),
        in_specs=[
            block(memory_space=pltpu.SMEM),
            block((group, span, heads * head_dim), lambda p: (p, 0, 0)),
            block((nf, group, heads, per, head_dim), lambda p: (0, p, 0, 0, 0)),
            block((group, heads, FD + 1, head_dim), lambda p: (p, 0, 0, 0)),
            block((group, H, per), lambda p: (p, 0, 0)),
            block((group, heads, FD + 1), lambda p: (p, 0, 0)),
        ],
        out_specs=[
            block((group, span, heads * head_dim), lambda p: (p, 0, 0)),
            block((group, H, per, head_dim), lambda p: (p, 0, 0, 0)),
            block((group, FD + 1, heads, head_dim), lambda p: (p, 0, 0, 0)),
            block((group, H, per), lambda p: (p, 0, 0)),
            block((group, heads, FD + 1), lambda p: (p, 0, 0)),
        ],
        name="finish",
    )(owners, mixed, quad, low, nq, nl)
    return (mixed, quad[None], jnp.transpose(low, (0, 2, 1, 3))[None], nq[None], nl[None])


def solution(mesh):
    placed = (P(None, "seq", None), P(), P(), P(None, "feat"), P(), P())
    return jax.shard_map(
        body,
        mesh=mesh,
        in_specs=placed,
        out_specs=(
            P(None, "seq", "feat"),
            P("seq", None, None, "feat", None),
            P("seq", None, "feat", None, None),
            P("seq", None, None, "feat"),
            P("seq", None, "feat", None),
        ),
        check_vma=False,
    )
```
